32 devices in a mesh: groups: 2 (over x), sp: 8 (over z, y), fsdp: 2 (over core).
Axes of the slice: x: 2, y: 2, z: 4, core: 2. Of those that a mesh axis runs over, the one named last changes fastest.
Arguments:
- policy_hidden: bfloat16 [4, 256, 4096], P(('groups', 'fsdp'), 'sp'), parts along dimension 0, may hold values from -6 to 6
- policy_queries: bfloat16 [4, 256, 1024], P(('groups', 'fsdp'), 'sp'), parts along dimension 0, may hold values from -512 to 512
- policy_documents: int32 [4, 256], P(('groups', 'fsdp'), 'sp'), parts along dimension 0, may hold values from 0 to 31, never falling along the last dimension, each value on 1 to 128 neighbouring positions
- policy_gain: bfloat16 [4096], P(('sp', 'fsdp')), may hold values from 0.099609375 to 1.8984375
- policy_key_weight: bfloat16 [4096, 512], P(('sp', 'fsdp')), may hold values from -0.09375 to 0.09375
- policy_value_weight: bfloat16 [4096, 512], P(('sp', 'fsdp')), may hold values from -0.09375 to 0.09375
- frozen_hidden: bfloat16 [4, 256, 4096], P(('groups', 'fsdp'), 'sp'), parts along dimension 0, may hold values from -6 to 6
- frozen_queries: bfloat16 [4, 256, 1024], P(('groups', 'fsdp'), 'sp'), parts along dimension 0, may hold values from -512 to 512
- frozen_documents: int32 [4, 256], P(('groups', 'fsdp'), 'sp'), parts along dimension 0, may hold values from 0 to 31, never falling along the last dimension, each value on 1 to 128 neighbouring positions
- frozen_gain: bfloat16 [4096], P(('sp', 'fsdp')), may hold values from 0.099609375 to 1.8984375
- frozen_key_weight: bfloat16 [4096, 512], P(('sp', 'fsdp')), may hold values from -0.09375 to 0.09375
- frozen_value_weight: bfloat16 [4096, 512], P(('sp', 'fsdp')), may hold values from -0.09375 to 0.09375
Outputs:
- policy_mixed: bfloat16 [4, 256, 1024], P(('groups', 'fsdp'), 'sp'), parts along dimension 0
- frozen_mixed: bfloat16 [4, 256, 1024], P(('groups', 'fsdp'), 'sp'), parts along dimension 0
The draws below stay inside these ranges and needn't reach their ends.
There are 2 independent parts, one for each index of `groups`. The reference program is written for one: setup_inputs(seed, part) draws one part's arguments, and reference() takes and returns one part's arrays. A program takes and returns all parts, laid end to end along the dimension named above; an argument that names none is the same for every part. Nothing has to cross between parts.
Inputs may be any that keep to these rules, and one draw needn't show every extreme that they name: `policy_documents`: along each sequence the ids never fall, and each document holds 1 to 128 positions. `frozen_documents`: along each sequence the ids never fall, and each document holds 1 to 128 positions.
All inputs are finite; a program needn't handle non-finite values.
Results may differ from the reference program's by a relative error of at most 0.007.
The reference program's roundings to bfloat16 on the way count: a program that leaves them out, or rounds other values in their place, can miss the bound.
Values may be sent and summed in bfloat16 or wider, within the bound.
A program may use at most 128 MiB of HBM per device.

```python
import math
import jax
import jax.numpy as jnp
import numpy as np
from jax import lax

D = 4096
HEAD_DIM = 128
KV_HEADS = 4
DOCS = 32
HEADS = 8
LENGTH = 256
DOC_MOST = 128
SEQS = 2


def query_draw(seed_key):
    standard = jax.random.normal(seed_key, (SEQS, LENGTH, HEADS, HEAD_DIM), jnp.float32)
    drawn = 2.5 * standard
    return jnp.clip(drawn, -512.0, 512.0).reshape(SEQS, LENGTH, HEADS * HEAD_DIM).astype(jnp.bfloat16)


def draw_policy_queries(key, part):
    return query_draw(jax.random.fold_in(key, 11))


def draw_frozen_queries(key, part):
    return query_draw(jax.random.fold_in(key, 23))


def levels(stream_key, dims, pieces, least, high):
    level, own = 1.0, jax.random.fold_in(stream_key, 6)
    for dim, blocks in pieces:
        steps = jnp.exp(jax.random.uniform(jax.random.fold_in(own, dim), (blocks,), jnp.float32, least / len(pieces), high / len(pieces)))
        level = level * jnp.repeat(steps, dims[dim] // blocks).reshape([-1 if axis == dim else 1 for axis in range(len(dims))])
    return level


def split_up(amount, total, limit, skew):
    portions = [(1 << 20) // math.isqrt(rank ** skew) + 1 for rank in range(2, amount + 1)]
    rest, counts = total - limit - (amount - 1), [1] * (amount - 1)
    while rest > 0:
        movable = [i for i in range(amount - 1) if counts[i] < limit]
        whole, budget = sum([portions[i] for i in movable]), rest
        for i in movable:
            extra = min(limit - counts[i], max(1, budget * portions[i] // whole), rest)
            counts[i] = counts[i] + extra
            rest = rest - extra
    return np.array([limit] + counts)


def ragged_sizes(own_key, count, total, bound, skew):
    if count == 2:
        one = jax.random.randint(own_key, (), max(1, total - bound), min(bound, total - 1) + 1)
        return jnp.stack([one, total - one])
    sizes = jnp.asarray(split_up(count, total, bound, skew), jnp.int32)
    pairs = (count - 1) // 2
    donor, sink = sizes[1:1 + 2 * pairs:2], sizes[2:2 + 2 * pairs:2]
    room = jnp.minimum(donor - 1, bound - sink)
    moved = jax.random.randint(jax.random.fold_in(own_key, 1), (pairs,), 0, 1 << 20) % (room + 1)
    sizes = sizes.at[1:1 + 2 * pairs:2].set(donor - moved).at[2:2 + 2 * pairs:2].set(sink + moved)
    return sizes[jax.random.permutation(jax.random.fold_in(own_key, 2), count)]


def bell_draw(key, shape, scale, reach, shards=(), kind=jnp.bfloat16):
    entries = scale * jax.random.normal(key, shape, jnp.float32)
    if shards:
        entries = entries * levels(key, shape, shards, -0.22, 0.18)
    return jnp.clip(entries, -reach, reach).astype(kind)


def setup_inputs(seed: int = 0, part: int = 0) -> dict:
    seeds = jax.random.split(jax.random.key(seed), 13)
    part_keys = jax.random.split(jax.random.fold_in(seeds[12], part), 13)
    policy_hidden = bell_draw(part_keys[0], (SEQS, LENGTH, D), 1.0, 6.0, ((0, 2), (1, 8)))
    policy_queries = draw_policy_queries(jax.random.fold_in(jax.random.fold_in(seeds[12], part), 71), part)
    policy_documents = jax.vmap(lambda own: jnp.searchsorted(jnp.cumsum(ragged_sizes(own, DOCS, LENGTH, DOC_MOST, 1)), jnp.arange(LENGTH), side="right"))(jax.random.split(part_keys[2], SEQS)).reshape((SEQS, LENGTH)).astype(jnp.int32)
    policy_gain = jnp.clip(1.0 + 0.18 * jax.random.normal(seeds[3], (D,), jnp.float32), 0.099609375, 1.8984375).astype(jnp.bfloat16)
    policy_key_weight = bell_draw(seeds[4], (D, KV_HEADS * HEAD_DIM), D ** -0.5, 0.09375, ((0, 16),))
    policy_value_weight = bell_draw(seeds[5], (D, KV_HEADS * HEAD_DIM), D ** -0.5, 0.09375, ((0, 16),))
    frozen_hidden = bell_draw(part_keys[6], (SEQS, LENGTH, D), 1.0, 6.0, ((0, 2), (1, 8)))
    frozen_queries = draw_frozen_queries(jax.random.fold_in(jax.random.fold_in(seeds[12], part), 71), part)
    frozen_documents = jax.vmap(lambda own: jnp.searchsorted(jnp.cumsum(ragged_sizes(own, DOCS, LENGTH, DOC_MOST, 1)), jnp.arange(LENGTH), side="right"))(jax.random.split(part_keys[8], SEQS)).reshape((SEQS, LENGTH)).astype(jnp.int32)
    frozen_gain = jnp.clip(1.0 + 0.18 * jax.random.normal(seeds[9], (D,), jnp.float32), 0.099609375, 1.8984375).astype(jnp.bfloat16)
    frozen_key_weight = bell_draw(seeds[10], (D, KV_HEADS * HEAD_DIM), D ** -0.5, 0.09375, ((0, 16),))
    frozen_value_weight = bell_draw(seeds[11], (D, KV_HEADS * HEAD_DIM), D ** -0.5, 0.09375, ((0, 16),))
    return {"policy_hidden": policy_hidden, "policy_queries": policy_queries, "policy_documents": policy_documents, "policy_gain": policy_gain, "policy_key_weight": policy_key_weight, "policy_value_weight": policy_value_weight, "frozen_hidden": frozen_hidden, "frozen_queries": frozen_queries, "frozen_documents": frozen_documents, "frozen_gain": frozen_gain, "frozen_key_weight": frozen_key_weight, "frozen_value_weight": frozen_value_weight}


EPS = 1e-05
ROPE_BASE = 500000.0
MASKED = -1e+30

def rotate(raw_keys, positions):
    half_dim = HEAD_DIM // 2
    frequency = jnp.exp(-jnp.log(ROPE_BASE) * jnp.arange(half_dim, dtype=jnp.float32) * 2.0 / HEAD_DIM)
    angles = positions.astype(jnp.float32)[:, None] * frequency[None, :]
    cosines = jnp.cos(angles)[:, None, :]
    sines = jnp.sin(angles)[:, None, :]
    front_half = raw_keys[..., :half_dim]
    back_half = raw_keys[..., half_dim:]
    return jnp.concatenate([front_half * cosines - back_half * sines, back_half * cosines + front_half * sines], axis=-1)

def one_model(hidden, queries, documents, gain, key_weight, value_weight):
    group_size = HEADS // KV_HEADS
    factor = HEAD_DIM ** (-0.5)
    block_rows = min(512, LENGTH)
    margin = min(512, LENGTH // 2)
    window = block_rows + margin

    def one_sequence(inputs):
        sequence, query_rows, doc_row = inputs
        widened = sequence.astype(jnp.float32)
        inverse = lax.rsqrt(lax.optimization_barrier(jnp.mean(widened * widened, axis=-1, keepdims=True)) + EPS)
        normed = (widened * inverse * gain.astype(jnp.float32)[None, :]).astype(jnp.bfloat16)
        positions = jnp.arange(LENGTH, dtype=jnp.int32)
        raw_keys = jnp.dot(normed, key_weight, preferred_element_type=jnp.float32).reshape(LENGTH, KV_HEADS, HEAD_DIM)
        key_heads = rotate(raw_keys, positions).astype(jnp.bfloat16)
        value_heads = jnp.dot(normed, value_weight, preferred_element_type=jnp.float32).astype(jnp.bfloat16).reshape(LENGTH, KV_HEADS, HEAD_DIM)
        query_heads = query_rows.reshape(LENGTH, HEADS, HEAD_DIM)
        padding = jnp.zeros((margin, KV_HEADS, HEAD_DIM), jnp.bfloat16)
        padded_keys = jnp.concatenate([padding, key_heads], axis=0)
        padded_values = jnp.concatenate([padding, value_heads], axis=0)
        padded_docs = jnp.concatenate([jnp.full((margin,), -1, jnp.int32), doc_row.astype(jnp.int32)], axis=0)
        offsets = jnp.arange(block_rows, dtype=jnp.int32)
        window_offsets = jnp.arange(window, dtype=jnp.int32)

        def one_block(block_index):
            first = (block_index * block_rows).astype(jnp.int32)
            query_block = lax.dynamic_slice_in_dim(query_heads, first, block_rows, 0).astype(jnp.float32)
            query_docs = lax.dynamic_slice_in_dim(doc_row.astype(jnp.int32), first, block_rows, 0)
            query_positions = first + offsets
            key_block = lax.dynamic_slice_in_dim(padded_keys, first, window, 0)
            value_block = lax.dynamic_slice_in_dim(padded_values, first, window, 0)
            key_docs = lax.dynamic_slice_in_dim(padded_docs, first, window, 0)
            key_positions = first - margin + window_offsets
            allowed = (key_positions[None, :] <= query_positions[:, None]) & (key_docs[None, :] == query_docs[:, None])
            wide_keys = jnp.repeat(key_block, group_size, axis=1).astype(jnp.float32)
            wide_values = jnp.repeat(value_block, group_size, axis=1).astype(jnp.float32)
            scores = jnp.einsum('qnd,knd->nqk', query_block, wide_keys) * factor
            scores = jnp.where(allowed[None], scores, MASKED)
            highest = lax.optimization_barrier(jnp.max(scores, axis=-1, keepdims=True))
            exponent = jnp.where(allowed[None], jnp.exp(scores - highest), 0.0)
            weights = (exponent / lax.optimization_barrier(jnp.sum(exponent, axis=-1, keepdims=True))).astype(jnp.bfloat16)
            return jnp.einsum('nqk,knd->qnd', weights.astype(jnp.float32), wide_values).astype(jnp.bfloat16)
        blocks = lax.map(one_block, jnp.arange(LENGTH // block_rows, dtype=jnp.int32))
        return blocks.reshape(LENGTH, HEADS * HEAD_DIM)
    return lax.map(one_sequence, (hidden, queries, documents))

def reference(policy_hidden, policy_queries, policy_documents, policy_gain, policy_key_weight, policy_value_weight, frozen_hidden, frozen_queries, frozen_documents, frozen_gain, frozen_key_weight, frozen_value_weight):
    policy_mixed = one_model(policy_hidden, policy_queries, policy_documents, policy_gain, policy_key_weight, policy_value_weight)
    frozen_mixed = one_model(frozen_hidden, frozen_queries, frozen_documents, frozen_gain, frozen_key_weight, frozen_value_weight)
    return (policy_mixed, frozen_mixed)
```

```python
import functools

import jax
import jax.numpy as jnp
from jax import lax
from jax.experimental import pallas as pl
from jax.experimental.pallas import tpu as pltpu
from jax.sharding import PartitionSpec as P

HEAD_DIM = 128


EPS = 1e-05
ROPE_BASE = 500000.0
MASKED = -1e30


def rotate(raw_keys, positions):
    half_dim = HEAD_DIM // 2
    frequency = jnp.exp(
        -jnp.log(ROPE_BASE) * jnp.arange(half_dim, dtype=jnp.float32) * 2.0 / HEAD_DIM
    )
    angles = positions.astype(jnp.float32)[:, None] * frequency[None, :]
    cosines = jnp.cos(angles)[:, None, :]
    sines = jnp.sin(angles)[:, None, :]
    front_half = raw_keys[..., :half_dim]
    back_half = raw_keys[..., half_dim:]
    return jnp.concatenate(
        [front_half * cosines - back_half * sines, back_half * cosines + front_half * sines],
        axis=-1,
    )


def project(hidden, gain, key_weight, value_weight):
    tokens = hidden.shape[1]
    widened = hidden[0].astype(jnp.float32)
    inverse = lax.rsqrt(jnp.mean(widened * widened, axis=-1, keepdims=True) + EPS)
    scaled = widened * inverse
    gain_rows = lax.all_gather(gain, ("sp", "fsdp"), axis=0, tiled=True)
    key_rows = lax.all_gather(key_weight, ("sp", "fsdp"), axis=0, tiled=True)
    value_rows = lax.all_gather(value_weight, ("sp", "fsdp"), axis=0, tiled=True)
    normed = (scaled * gain_rows.astype(jnp.float32)[None, :]).astype(jnp.bfloat16)
    raw_keys = jnp.dot(normed, key_rows, preferred_element_type=jnp.float32)
    raw_values = jnp.dot(normed, value_rows, preferred_element_type=jnp.float32)
    positions = lax.axis_index("sp") * tokens + jnp.arange(tokens, dtype=jnp.int32)
    key_heads = rotate(raw_keys.reshape(tokens, -1, HEAD_DIM), positions).astype(jnp.bfloat16)
    value_heads = raw_values.astype(jnp.bfloat16).reshape(tokens, -1, HEAD_DIM)
    return (key_heads, value_heads)


def attend(queries, key_heads, value_heads, documents):
    length = queries.shape[0]
    head_count = queries.shape[1]
    block_rows = min(512, length)
    margin = min(512, length // 2)
    window = block_rows + margin
    factor = HEAD_DIM ** (-0.5)
    offsets = jnp.arange(block_rows, dtype=jnp.int32)
    window_offsets = jnp.arange(window, dtype=jnp.int32)
    padding = jnp.zeros((margin, head_count, HEAD_DIM), jnp.bfloat16)
    padded_keys = jnp.concatenate([padding, key_heads], axis=0)
    padded_values = jnp.concatenate([padding, value_heads], axis=0)
    padded_docs = jnp.concatenate([jnp.full((margin,), -1, jnp.int32), documents], axis=0)

    def one_block(block_index):
        first = block_index * block_rows
        query_block = lax.dynamic_slice_in_dim(queries, first, block_rows, 0)
        query_docs = lax.dynamic_slice_in_dim(documents, first, block_rows, 0)
        query_positions = first + offsets
        key_block = lax.dynamic_slice_in_dim(padded_keys, first, window, 0)
        value_block = lax.dynamic_slice_in_dim(padded_values, first, window, 0)
        key_docs = lax.dynamic_slice_in_dim(padded_docs, first, window, 0)
        key_positions = first - margin + window_offsets
        allowed = (key_positions[None, :] <= query_positions[:, None]) & (
            key_docs[None, :] == query_docs[:, None]
        )
        scores = (
            jnp.einsum("qnd,knd->nqk", query_block, key_block, preferred_element_type=jnp.float32)
            * factor
        )
        scores = jnp.where(allowed[None], scores, MASKED)
        highest = jnp.max(scores, axis=-1, keepdims=True)
        exponent = jnp.where(allowed[None], jnp.exp(scores - highest), 0.0)
        weights = (exponent / jnp.sum(exponent, axis=-1, keepdims=True)).astype(jnp.bfloat16)
        blended = jnp.einsum(
            "nqk,knd->qnd", weights, value_block, preferred_element_type=jnp.float32
        )
        return blended.astype(jnp.bfloat16)

    blocks = lax.map(one_block, jnp.arange(length // block_rows, dtype=jnp.int32))
    return blocks.reshape(length, head_count, HEAD_DIM)


def run_model(hidden, queries, documents, gain, key_weight, value_weight):
    tokens = hidden.shape[1]
    head_count = queries.shape[2] // HEAD_DIM
    query_local = queries[0].reshape(tokens, head_count, HEAD_DIM)
    every_doc = lax.all_gather(documents[0], "sp", axis=0, tiled=True)
    key_heads, value_heads = project(hidden, gain, key_weight, value_weight)
    group_size = head_count // key_heads.shape[1]
    wide_keys = jnp.repeat(key_heads, group_size, axis=1)
    wide_values = jnp.repeat(value_heads, group_size, axis=1)
    query_spread, key_spread, value_spread = (
        lax.all_to_all(query_local, "sp", split_axis=1, concat_axis=0, tiled=True),
        lax.all_to_all(wide_keys, "sp", split_axis=1, concat_axis=0, tiled=True),
        lax.all_to_all(wide_values, "sp", split_axis=1, concat_axis=0, tiled=True),
    )
    mixed = attend(query_spread, key_spread, value_spread, every_doc)
    returned = lax.all_to_all(mixed, "sp", split_axis=0, concat_axis=1, tiled=True)
    return returned.reshape(1, tokens, head_count * HEAD_DIM)


MESH = pl.DeviceIdType.MESH


def fits(mesh, hidden, queries, key_weight):
    sp, cores = mesh.shape["sp"], mesh.shape["fsdp"]
    tokens = hidden.shape[1]
    kv_heads = key_weight.shape[1] // HEAD_DIM
    return (
        cores == 2
        and sp % 2 == 0
        and kv_heads % 2 == 0
        and sp // 2 == cores * (kv_heads // 2)
        and queries.shape[2] % (kv_heads * HEAD_DIM) == 0
        and key_weight.shape[0] % 128 == 0
        and hidden.shape[2] == key_weight.shape[0] * sp * cores
        and tokens % 16 == 0
        and tokens <= 128
    )


def fused_kernel(
    sp_count,
    hidden0, hidden1, queries0, queries1, key0, key1, value0, value1,
    gains, documents, cosines, sines,
    out,
    rows, wide_k, wide_v, gain_rows, norm_send, norm_rows, query_rows, doc_rows,
    part_send, parts, doc_wide, mixed,
    send_sem, hid_sem, fwd_sem, w_sem, gain_sem, norm_sem, q_sem, doc_sem, part_sem, out_sem,
):
    hiddens, queries = (hidden0, hidden1), (queries0, queries1)
    keys, values = (key0, key1), (value0, value1)
    tokens, features = hidden0.shape[1], key0.shape[0]
    slab = 4 * features
    half = key0.shape[1] // 2
    per_half = half // HEAD_DIM
    head_cols = query_rows.shape[1]
    length = query_rows.shape[0]
    layers = sp_count // 2
    sp, core = lax.axis_index("sp"), lax.axis_index("fsdp")
    z, y = sp // 2, sp % 2
    me = sp * 2 + core
    total = sp_count * 2

    barrier = pltpu.get_barrier_semaphore()
    for step in range(1, total):
        other = lax.rem(me + step, total)
        pl.semaphore_signal(
            barrier, inc=1, device_id={"sp": other // 2, "fsdp": other % 2}, device_id_type=MESH
        )

    square = (
        lax.broadcasted_iota(jnp.int32, (tokens, 128), 0)
        == lax.broadcasted_iota(jnp.int32, (tokens, 128), 1)
    )
    for m in range(2):
        wide = hiddens[m][0].astype(jnp.float32)
        inverse = lax.rsqrt(jnp.mean(wide * wide, axis=-1, keepdims=True) + EPS)
        norm_send[m] = jnp.sum(jnp.where(square, inverse, 0.0), axis=0, keepdims=True)

    pl.semaphore_wait(barrier, total - 1)

    pending = []

    def remote(src, dst, recv, to_sp, to_core):
        slot = len(pending)

        def make():
            return pltpu.make_async_remote_copy(
                src_ref=src, dst_ref=dst, send_sem=send_sem.at[slot], recv_sem=recv,
                device_id={"sp": to_sp, "fsdp": to_core}, device_id_type=MESH,
            )

        return make

    def send(src, dst, recv, to_sp, to_core, own):
        make = remote(src, dst, recv, to_sp, to_core)
        if own is None:
            pending.append((None, make))
            make().start()
            return
        away = jnp.logical_not(own)
        pending.append((away, make))

        @pl.when(away)
        def _():
            make().start()

        @pl.when(own)
        def _():
            pltpu.make_async_copy(src, dst, recv).start()

    def arrive(dst, recv):
        pltpu.make_async_copy(dst, dst, recv).wait()

    for dz in range(layers):
        to_z = lax.rem(z + dz, layers)
        for m in range(2):
            send(
                hiddens[m].at[0, :, pl.ds(pl.multiple_of(to_z * slab, 128), slab)],
                rows.at[sp, pl.ds(pl.multiple_of(core * tokens, 16), tokens)],
                hid_sem.at[z, core],
                to_z * 2 + y, m,
                (core == m) if dz == 0 else None,
            )
    place = pl.ds(pl.multiple_of((y * 2 + core) * features, 128), features)
    for dy in (1, 0):
        to_y = (y + dy) % 2
        columns = pl.ds(pl.multiple_of(to_y * half, 128), half)
        for m in range(2):
            own = (core == m) if dy == 0 else None
            send(gains.at[m], gain_rows.at[y * 2 + core], gain_sem.at[y * 2 + core], z * 2 + to_y, m, own)
            send(keys[m].at[:, columns], wide_k.at[place], w_sem.at[y * 2 + core, 0], z * 2 + to_y, m, own)
            send(values[m].at[:, columns], wide_v.at[place], w_sem.at[y * 2 + core, 1], z * 2 + to_y, m, own)
    for dz in range(layers):
        for dy in range(2):
            to_sp = lax.rem(z + dz, layers) * 2 + (y + dy) % 2
            for m in range(2):
                send(
                    norm_send.at[m], norm_rows.at[me], norm_sem.at[me], to_sp, m,
                    (core == m) if dz == 0 and dy == 0 else None,
                )
    token_rows = pl.ds(pl.multiple_of(sp * tokens, 16), tokens)
    for b in range(per_half):
        for to_y in range(2):
            head = to_y * per_half + b
            to_sp = (core * per_half + b) * 2 + to_y
            for m in range(2):
                own = (to_sp == sp) & (core == m)
                send(
                    queries[m].at[0, :, head * head_cols:(head + 1) * head_cols],
                    query_rows.at[token_rows], q_sem.at[sp], to_sp, m, own,
                )
                send(documents.at[m], doc_rows.at[sp], doc_sem.at[sp], to_sp, m, own)

    for dz in range(layers):
        from_z = lax.rem(z - dz + layers, layers)
        block = from_z * 2 + y
        for c in range(2):
            arrive(rows.at[block, c * tokens:(c + 1) * tokens], hid_sem.at[from_z, c])
        send(rows.at[block], rows.at[block], fwd_sem.at[from_z], z * 2 + (1 - y), core, None)

    for s in range(total):
        arrive(norm_rows.at[s], norm_sem.at[s])
    for s in range(4):
        arrive(gain_rows.at[s], gain_sem.at[s])
        arrive(wide_k.at[s * features:(s + 1) * features], w_sem.at[s, 0])
        arrive(wide_v.at[s * features:(s + 1) * features], w_sem.at[s, 1])
    gain_row = jnp.concatenate([gain_rows[s] for s in range(4)], axis=1)

    for side in range(2):
        for dz in range(layers):
            from_z = lax.rem(z - dz + layers, layers)
            block = from_z * 2 + (y + side) % 2
            if side:
                arrive(rows.at[block], fwd_sem.at[from_z])
            scale = jnp.concatenate(
                [
                    jnp.sum(jnp.where(square, norm_rows[block * 2 + c], 0.0), axis=1, keepdims=True)
                    for c in range(2)
                ],
                axis=0,
            )
            normed = (rows[block].astype(jnp.float32) * scale * gain_row).astype(jnp.bfloat16)
            part_k = jnp.dot(normed, wide_k[...], preferred_element_type=jnp.float32)
            part_v = jnp.dot(normed, wide_v[...], preferred_element_type=jnp.float32)
            block_rows = pl.ds(pl.multiple_of(block * tokens, 16), tokens)
            for s in range(2):
                for b in range(per_half):
                    to_z = s * per_half + b
                    own = z == to_z
                    picked = (slice(s * tokens, (s + 1) * tokens), slice(b * HEAD_DIM, (b + 1) * HEAD_DIM))
                    slot = (side * layers + dz) * layers + to_z
                    part_send[slot, :, :HEAD_DIM] = part_k[picked]
                    part_send[slot, :, HEAD_DIM:] = part_v[picked]
                    make = remote(
                        part_send.at[slot], parts.at[z, block_rows], part_sem.at[z, block], to_z * 2 + y, core
                    )
                    away = jnp.logical_not(own)
                    pending.append((away, make))

                    @pl.when(away)
                    def _(make=make):
                        make().start()

                    @pl.when(own)
                    def _(slot=slot, block_rows=block_rows):
                        parts[z, block_rows, :] = part_send[slot]

    for s in range(sp_count):
        arrive(query_rows.at[s * tokens:(s + 1) * tokens], q_sem.at[s])
        arrive(doc_rows.at[s], doc_sem.at[s])
        column = jnp.sum(jnp.where(square, doc_rows[s], 0.0), axis=1, keepdims=True)
        doc_wide[s * tokens:(s + 1) * tokens, :] = jnp.broadcast_to(column, (tokens, 128))
    query_index = lax.broadcasted_iota(jnp.int32, (length, length), 0)
    key_index = lax.broadcasted_iota(jnp.int32, (length, length), 1)
    doc_column = doc_wide[:, :1]
    doc_row = jnp.sum(jnp.where(query_index == key_index, doc_column, 0.0), axis=0, keepdims=True)
    allowed = (key_index <= query_index) & (doc_row == doc_column)

    for from_z in range(layers):
        @pl.when(z != from_z)
        def _(from_z=from_z):
            for s in range(sp_count):
                arrive(parts.at[from_z, s * tokens:(s + 1) * tokens], part_sem.at[from_z, s])
    raw = parts[0]
    for from_z in range(1, layers):
        raw = raw + parts[from_z]
    raw_keys = raw[:, :HEAD_DIM]
    key_heads = (
        raw_keys * cosines[...] + pltpu.roll(raw_keys, HEAD_DIM // 2, 1) * sines[...]
    ).astype(jnp.bfloat16)
    value_heads = raw[:, HEAD_DIM:].astype(jnp.bfloat16)
    factor = HEAD_DIM ** (-0.5)
    for g in range(head_cols // HEAD_DIM):
        columns = slice(g * HEAD_DIM, (g + 1) * HEAD_DIM)
        scores = lax.dot_general(
            query_rows[:, columns], key_heads, (((1,), (1,)), ((), ())), preferred_element_type=jnp.float32
        ) * factor
        scores = jnp.where(allowed, scores, MASKED)
        highest = jnp.max(scores, axis=-1, keepdims=True)
        exponent = jnp.where(allowed, jnp.exp(scores - highest), 0.0)
        weights = (exponent / jnp.sum(exponent, axis=-1, keepdims=True)).astype(jnp.bfloat16)
        mixed[:, columns] = jnp.dot(weights, value_heads, preferred_element_type=jnp.float32).astype(jnp.bfloat16)

    my_seq, my_head = z // per_half, y * per_half + z % per_half
    out_columns = pl.ds(pl.multiple_of(my_head * head_cols, 128), head_cols)
    for s in range(sp_count):
        send(
            mixed.at[s * tokens:(s + 1) * tokens], out.at[core, :, out_columns],
            out_sem.at[core, my_head], s, my_seq, (sp == s) & (core == my_seq),
        )
    for m in range(2):
        for head in range(2 * per_half):
            arrive(out.at[m, :, head * head_cols:(head + 1) * head_cols], out_sem.at[m, head])
    for away, make in pending:
        if away is None:
            make().wait_send()
        else:
            @pl.when(away)
            def _(make=make):
                make().wait_send()


def fused(mesh, hiddens, queries, documents, gains, keys, values):
    sp = mesh.shape["sp"]
    tokens, features = hiddens[0].shape[1], keys[0].shape[0]
    kv_heads = keys[0].shape[1] // HEAD_DIM
    head_cols = queries[0].shape[2] // kv_heads
    layers, length, half = sp // 2, sp * tokens, keys[0].shape[1] // 2
    half_dim = HEAD_DIM // 2
    frequency = jnp.exp(
        -jnp.log(ROPE_BASE) * jnp.arange(half_dim, dtype=jnp.float32) * 2.0 / HEAD_DIM
    )
    angles = jnp.arange(length, dtype=jnp.int32).astype(jnp.float32)[:, None] * frequency[None, :]
    cosines, sines = jnp.cos(angles), jnp.sin(angles)
    cosines = jnp.concatenate([cosines, cosines], axis=1)
    sines = jnp.concatenate([-sines, sines], axis=1)
    gain_pair = jnp.stack(gains)[:, None, :].astype(jnp.float32)
    doc_pair = jnp.pad(jnp.stack(documents).astype(jnp.float32), ((0, 0), (0, 0), (0, 128 - tokens)))
    dma = pltpu.SemaphoreType.DMA
    bf16, f32 = jnp.bfloat16, jnp.float32
    sends = 2 * layers + 12 + 4 * layers + 4 * kv_heads + layers + sp * layers + sp
    out = pl.pallas_call(
        functools.partial(fused_kernel, sp),
        out_shape=jax.ShapeDtypeStruct((2, tokens, queries[0].shape[2]), bf16),
        in_specs=[pl.BlockSpec(memory_space=pltpu.VMEM)] * 12,
        out_specs=pl.BlockSpec(memory_space=pltpu.VMEM),
        scratch_shapes=[
            pltpu.VMEM((sp, 2 * tokens, 4 * features), bf16),
            pltpu.VMEM((4 * features, half), bf16),
            pltpu.VMEM((4 * features, half), bf16),
            pltpu.VMEM((4, 1, features), f32),
            pltpu.VMEM((2, 1, 128), f32),
            pltpu.VMEM((2 * sp, 1, 128), f32),
            pltpu.VMEM((length, head_cols), bf16),
            pltpu.VMEM((sp, 1, 128), f32),
            pltpu.VMEM((sp * layers, tokens, 2 * HEAD_DIM), f32),
            pltpu.VMEM((layers, length, 2 * HEAD_DIM), f32),
            pltpu.VMEM((length, 128), f32),
            pltpu.VMEM((length, head_cols), bf16),
            dma((sends,)),
            dma((layers, 2)),
            dma((layers,)),
            dma((4, 2)),
            dma((4,)),
            dma((2 * sp,)),
            dma((sp,)),
            dma((sp,)),
            dma((layers, sp)),
            dma((2, kv_heads)),
        ],
        compiler_params=pltpu.CompilerParams(collective_id=0, has_side_effects=True),
        name="fused",
    )(*hiddens, *queries, *keys, *values, gain_pair, doc_pair, cosines, sines)
    return (out[0][None], out[1][None])


def per_device(
    mesh,
    policy_hidden,
    policy_queries,
    policy_documents,
    policy_gain,
    policy_key_weight,
    policy_value_weight,
    frozen_hidden,
    frozen_queries,
    frozen_documents,
    frozen_gain,
    frozen_key_weight,
    frozen_value_weight,
):
    if fits(mesh, policy_hidden, policy_queries, policy_key_weight):
        return fused(
            mesh,
            (policy_hidden, frozen_hidden),
            (policy_queries, frozen_queries),
            (policy_documents, frozen_documents),
            (policy_gain, frozen_gain),
            (policy_key_weight, frozen_key_weight),
            (policy_value_weight, frozen_value_weight),
        )
    policy_mixed = run_model(
        policy_hidden,
        policy_queries,
        policy_documents,
        policy_gain,
        policy_key_weight,
        policy_value_weight,
    )
    frozen_mixed = run_model(
        frozen_hidden,
        frozen_queries,
        frozen_documents,
        frozen_gain,
        frozen_key_weight,
        frozen_value_weight,
    )
    return (policy_mixed, frozen_mixed)


def solution(mesh):
    return jax.shard_map(
        functools.partial(per_device, mesh),
        mesh=mesh,
        in_specs=(
            P(("groups", "fsdp"), "sp", None),
            P(("groups", "fsdp"), "sp", None),
            P(("groups", "fsdp"), "sp"),
            P(("sp", "fsdp")),
            P(("sp", "fsdp"), None),
            P(("sp", "fsdp"), None),
            P(("groups", "fsdp"), "sp", None),
            P(("groups", "fsdp"), "sp", None),
            P(("groups", "fsdp"), "sp"),
            P(("sp", "fsdp")),
            P(("sp", "fsdp"), None),
            P(("sp", "fsdp"), None),
        ),
        out_specs=(P(("groups", "fsdp"), "sp", None), P(("groups", "fsdp"), "sp", None)),
        check_vma=False,
    )
```

```python
import functools

import jax
import jax.numpy as jnp
import numpy as np
from jax import lax
from jax.experimental import pallas as pl
from jax.experimental.pallas import tpu as pltpu
from jax.sharding import PartitionSpec as P

HEAD_DIM = 128


EPS = 1e-05
ROPE_BASE = 500000.0
MASKED = -1e30


def rotate(raw_keys, positions):
    half_dim = HEAD_DIM // 2
    frequency = jnp.exp(
        -jnp.log(ROPE_BASE) * jnp.arange(half_dim, dtype=jnp.float32) * 2.0 / HEAD_DIM
    )
    angles = positions.astype(jnp.float32)[:, None] * frequency[None, :]
    cosines = jnp.cos(angles)[:, None, :]
    sines = jnp.sin(angles)[:, None, :]
    front_half = raw_keys[..., :half_dim]
    back_half = raw_keys[..., half_dim:]
    return jnp.concatenate(
        [front_half * cosines - back_half * sines, back_half * cosines + front_half * sines],
        axis=-1,
    )


def project(hidden, gain, key_weight, value_weight):
    tokens = hidden.shape[1]
    widened = hidden[0].astype(jnp.float32)
    inverse = lax.rsqrt(jnp.mean(widened * widened, axis=-1, keepdims=True) + EPS)
    scaled = widened * inverse
    gain_rows = lax.all_gather(gain, ("sp", "fsdp"), axis=0, tiled=True)
    key_rows = lax.all_gather(key_weight, ("sp", "fsdp"), axis=0, tiled=True)
    value_rows = lax.all_gather(value_weight, ("sp", "fsdp"), axis=0, tiled=True)
    normed = (scaled * gain_rows.astype(jnp.float32)[None, :]).astype(jnp.bfloat16)
    raw_keys = jnp.dot(normed, key_rows, preferred_element_type=jnp.float32)
    raw_values = jnp.dot(normed, value_rows, preferred_element_type=jnp.float32)
    positions = lax.axis_index("sp") * tokens + jnp.arange(tokens, dtype=jnp.int32)
    key_heads = rotate(raw_keys.reshape(tokens, -1, HEAD_DIM), positions).astype(jnp.bfloat16)
    value_heads = raw_values.astype(jnp.bfloat16).reshape(tokens, -1, HEAD_DIM)
    return (key_heads, value_heads)


def attend(queries, key_heads, value_heads, documents):
    length = queries.shape[0]
    head_count = queries.shape[1]
    block_rows = min(512, length)
    margin = min(512, length // 2)
    window = block_rows + margin
    factor = HEAD_DIM ** (-0.5)
    offsets = jnp.arange(block_rows, dtype=jnp.int32)
    window_offsets = jnp.arange(window, dtype=jnp.int32)
    padding = jnp.zeros((margin, head_count, HEAD_DIM), jnp.bfloat16)
    padded_keys = jnp.concatenate([padding, key_heads], axis=0)
    padded_values = jnp.concatenate([padding, value_heads], axis=0)
    padded_docs = jnp.concatenate([jnp.full((margin,), -1, jnp.int32), documents], axis=0)

    def one_block(block_index):
        first = block_index * block_rows
        query_block = lax.dynamic_slice_in_dim(queries, first, block_rows, 0)
        query_docs = lax.dynamic_slice_in_dim(documents, first, block_rows, 0)
        query_positions = first + offsets
        key_block = lax.dynamic_slice_in_dim(padded_keys, first, window, 0)
        value_block = lax.dynamic_slice_in_dim(padded_values, first, window, 0)
        key_docs = lax.dynamic_slice_in_dim(padded_docs, first, window, 0)
        key_positions = first - margin + window_offsets
        allowed = (key_positions[None, :] <= query_positions[:, None]) & (
            key_docs[None, :] == query_docs[:, None]
        )
        scores = (
            jnp.einsum("qnd,knd->nqk", query_block, key_block, preferred_element_type=jnp.float32)
            * factor
        )
        scores = jnp.where(allowed[None], scores, MASKED)
        highest = jnp.max(scores, axis=-1, keepdims=True)
        exponent = jnp.where(allowed[None], jnp.exp(scores - highest), 0.0)
        weights = (exponent / jnp.sum(exponent, axis=-1, keepdims=True)).astype(jnp.bfloat16)
        blended = jnp.einsum(
            "nqk,knd->qnd", weights, value_block, preferred_element_type=jnp.float32
        )
        return blended.astype(jnp.bfloat16)

    blocks = lax.map(one_block, jnp.arange(length // block_rows, dtype=jnp.int32))
    return blocks.reshape(length, head_count, HEAD_DIM)


def run_model(hidden, queries, documents, gain, key_weight, value_weight):
    tokens = hidden.shape[1]
    head_count = queries.shape[2] // HEAD_DIM
    query_local = queries[0].reshape(tokens, head_count, HEAD_DIM)
    every_doc = lax.all_gather(documents[0], "sp", axis=0, tiled=True)
    key_heads, value_heads = project(hidden, gain, key_weight, value_weight)
    group_size = head_count // key_heads.shape[1]
    wide_keys = jnp.repeat(key_heads, group_size, axis=1)
    wide_values = jnp.repeat(value_heads, group_size, axis=1)
    query_spread, key_spread, value_spread = (
        lax.all_to_all(query_local, "sp", split_axis=1, concat_axis=0, tiled=True),
        lax.all_to_all(wide_keys, "sp", split_axis=1, concat_axis=0, tiled=True),
        lax.all_to_all(wide_values, "sp", split_axis=1, concat_axis=0, tiled=True),
    )
    mixed = attend(query_spread, key_spread, value_spread, every_doc)
    returned = lax.all_to_all(mixed, "sp", split_axis=0, concat_axis=1, tiled=True)
    return returned.reshape(1, tokens, head_count * HEAD_DIM)


MESH = pl.DeviceIdType.MESH


def fits(mesh, hidden, queries, key_weight):
    sp, cores = mesh.shape["sp"], mesh.shape["fsdp"]
    tokens = hidden.shape[1]
    kv_heads = key_weight.shape[1] // HEAD_DIM
    return (
        cores == 2
        and mesh.shape["groups"] == 2
        and sp % 2 == 0
        and kv_heads % 2 == 0
        and sp // 2 == cores * (kv_heads // 2)
        and queries.shape[2] % (kv_heads * HEAD_DIM) == 0
        and key_weight.shape[0] % 128 == 0
        and hidden.shape[2] == key_weight.shape[0] * sp * cores
        and tokens % 16 == 0
        and tokens <= 128
    )


def fused_kernel(
    sp_count,
    hidden0, hidden1, queries0, queries1, key0, key1, value0, value1,
    gain0, gain1, documents0, documents1, cosines, sines,
    out0, out1,
    rows, wide_k, wide_v, gains, documents, gain_rows, norm_send, norm_rows, query_rows, doc_rows,
    part_send, parts, doc_wide, mixed,
    send_sem, hid_sem, fwd_sem, w_sem, gain_sem, norm_sem, q_sem, doc_sem, part_sem, out_sem,
):
    hiddens, queries = (hidden0, hidden1), (queries0, queries1)
    keys, values = (key0, key1), (value0, value1)
    tokens, features = hidden0.shape[1], key0.shape[0]
    slab = 4 * features
    half = key0.shape[1] // 2
    per_half = half // HEAD_DIM
    head_cols = query_rows.shape[1]
    length = query_rows.shape[0]
    layers = sp_count // 2
    sp, core = lax.axis_index("sp"), lax.axis_index("fsdp")
    z, y = sp // 2, sp % 2
    group = lax.axis_index("groups")
    me = sp * 2 + core
    total = sp_count * 2

    barrier = pltpu.get_barrier_semaphore()
    for step in range(1, total):
        other = lax.rem(me + step, total)
        pl.semaphore_signal(
            barrier, inc=1, device_id={"sp": other // 2, "fsdp": other % 2}, device_id_type=MESH
        )

    pl.semaphore_signal(barrier, inc=1, device_id={"groups": 1 - group}, device_id_type=MESH)

    square = (
        lax.broadcasted_iota(jnp.int32, (tokens, 128), 0)
        == lax.broadcasted_iota(jnp.int32, (tokens, 128), 1)
    )
    for m in range(2):
        wide = hiddens[m][0].astype(jnp.float32)
        inverse = lax.rsqrt(jnp.mean(wide * wide, axis=-1, keepdims=True) + EPS)
        gains[m] = (gain0, gain1)[m][...].astype(jnp.float32).reshape(1, -1)
        documents[m] = jnp.zeros((1, 128), jnp.float32)
        documents[m, :, :tokens] = (documents0, documents1)[m][...].astype(jnp.float32)
        norm_send[m] = jnp.sum(jnp.where(square, inverse, 0.0), axis=0, keepdims=True)

    pl.semaphore_wait(barrier, total)

    pending = []

    def remote(src, dst, recv, target):
        slot = len(pending)

        def make():
            return pltpu.make_async_remote_copy(
                src_ref=src, dst_ref=dst, send_sem=send_sem.at[slot], recv_sem=recv,
                device_id=target, device_id_type=MESH,
            )

        return make

    def put(src, dst, recv, target, away):
        make = remote(src, dst, recv, target)
        pending.append((away, make))
        if away is None:
            make().start()
        else:
            @pl.when(away)
            def _():
                make().start()

    def send(src, dst, recv, to_sp, to_core, own):
        put(src, dst, recv, {"sp": to_sp, "fsdp": to_core}, None if own is None else jnp.logical_not(own))
        if own is not None:
            @pl.when(own)
            def _():
                pltpu.make_async_copy(src, dst, recv).start()

    def arrive(dst, recv):
        pltpu.make_async_copy(dst, dst, recv).wait()

    for dz in range(layers):
        to_z = lax.rem(z + dz, layers)
        for m in range(2):
            send(
                hiddens[m].at[0, :, pl.ds(pl.multiple_of(to_z * slab, 128), slab)],
                rows.at[sp, pl.ds(pl.multiple_of(core * tokens, 16), tokens)],
                hid_sem.at[z, core],
                to_z * 2 + y, m,
                (core == m) if dz == 0 else None,
            )
    place = pl.ds(pl.multiple_of((y * 2 + core) * features, 128), features)
    for dy in (1, 0):
        to_y = (y + dy) % 2
        columns = pl.ds(pl.multiple_of(to_y * half, 128), half)
        for m in range(2):
            own = (core == m) if dy == 0 else None
            if dy:
                target = {"sp": z * 2 + to_y, "fsdp": m}
                put(keys[m].at[:, columns], wide_k.at[place], w_sem.at[y * 2 + core, 0], target, core == group)
                put(values[m].at[:, columns], wide_v.at[place], w_sem.at[y * 2 + core, 1], target, core == group)
            else:
                send(keys[m].at[:, columns], wide_k.at[place], w_sem.at[y * 2 + core, 0], z * 2 + to_y, m, own)
                send(values[m].at[:, columns], wide_v.at[place], w_sem.at[y * 2 + core, 1], z * 2 + to_y, m, own)
            send(gains.at[m], gain_rows.at[y * 2 + core], gain_sem.at[y * 2 + core], z * 2 + to_y, m, own)
    for dz in range(layers):
        for dy in range(2):
            to_sp = lax.rem(z + dz, layers) * 2 + (y + dy) % 2
            for m in range(2):
                send(
                    norm_send.at[m], norm_rows.at[me], norm_sem.at[me], to_sp, m,
                    (core == m) if dz == 0 and dy == 0 else None,
                )
    token_rows = pl.ds(pl.multiple_of(sp * tokens, 16), tokens)
    for b in range(per_half):
        for to_y in range(2):
            head = to_y * per_half + b
            to_sp = (core * per_half + b) * 2 + to_y
            for m in range(2):
                own = (to_sp == sp) & (core == m)
                send(
                    queries[m].at[0, :, head * head_cols:(head + 1) * head_cols],
                    query_rows.at[token_rows], q_sem.at[sp], to_sp, m, own,
                )
                send(documents.at[m], doc_rows.at[sp], doc_sem.at[sp], to_sp, m, own)

    for dz in range(layers):
        from_z = lax.rem(z - dz + layers, layers)
        block = from_z * 2 + y
        for c in range(2):
            arrive(rows.at[block, c * tokens:(c + 1) * tokens], hid_sem.at[from_z, c])
        send(rows.at[block], rows.at[block], fwd_sem.at[from_z], z * 2 + (1 - y), core, None)
        if dz < 2:
            source = (1 - y) * 2 + group
            wide = (wide_k, wide_v)[dz].at[pl.ds(pl.multiple_of(source * features, 128), features)]
            arrive(wide, w_sem.at[source, dz])
            put(wide, wide, w_sem.at[source, dz], {"groups": 1 - group}, None)

    for s in range(total):
        arrive(norm_rows.at[s], norm_sem.at[s])
    for s in range(4):
        arrive(gain_rows.at[s], gain_sem.at[s])
    for source in (y * 2, y * 2 + 1, (1 - y) * 2 + 1 - group):
        place = pl.ds(pl.multiple_of(source * features, 128), features)
        arrive(wide_k.at[place], w_sem.at[source, 0])
        arrive(wide_v.at[place], w_sem.at[source, 1])
    gain_row = jnp.concatenate([gain_rows[s] for s in range(4)], axis=1)

    for side in range(2):
        for dz in range(layers):
            from_z = lax.rem(z - dz + layers, layers)
            block = from_z * 2 + (y + side) % 2
            if side:
                arrive(rows.at[block], fwd_sem.at[from_z])
            scale = jnp.concatenate(
                [
                    jnp.sum(jnp.where(square, norm_rows[block * 2 + c], 0.0), axis=1, keepdims=True)
                    for c in range(2)
                ],
                axis=0,
            )
            normed = (rows[block].astype(jnp.float32) * scale * gain_row).astype(jnp.bfloat16)
            part_k = jnp.dot(normed, wide_k[...], preferred_element_type=jnp.float32)
            part_v = jnp.dot(normed, wide_v[...], preferred_element_type=jnp.float32)
            block_rows = pl.ds(pl.multiple_of(block * tokens, 16), tokens)
            for s in range(2):
                for b in range(per_half):
                    to_z = s * per_half + b
                    own = z == to_z
                    picked = (slice(s * tokens, (s + 1) * tokens), slice(b * HEAD_DIM, (b + 1) * HEAD_DIM))
                    slot = (side * layers + dz) * layers + to_z
                    part_send[slot, :, :HEAD_DIM] = part_k[picked]
                    part_send[slot, :, HEAD_DIM:] = part_v[picked]
                    make = remote(
                        part_send.at[slot], parts.at[z, block_rows], part_sem.at[z, block],
                        {"sp": to_z * 2 + y, "fsdp": core},
                    )
                    away = jnp.logical_not(own)
                    pending.append((away, make))

                    @pl.when(away)
                    def _(make=make):
                        make().start()

                    @pl.when(own)
                    def _(slot=slot, block_rows=block_rows):
                        parts[z, block_rows, :] = part_send[slot]

    for s in range(sp_count):
        arrive(query_rows.at[s * tokens:(s + 1) * tokens], q_sem.at[s])
        arrive(doc_rows.at[s], doc_sem.at[s])
        column = jnp.sum(jnp.where(square, doc_rows[s], 0.0), axis=1, keepdims=True)
        doc_wide[s * tokens:(s + 1) * tokens, :] = jnp.broadcast_to(column, (tokens, 128))
    query_index = lax.broadcasted_iota(jnp.int32, (length, length), 0)
    key_index = lax.broadcasted_iota(jnp.int32, (length, length), 1)
    doc_column = doc_wide[:, :1]
    doc_row = jnp.sum(jnp.where(query_index == key_index, doc_column, 0.0), axis=0, keepdims=True)
    allowed = (key_index <= query_index) & (doc_row == doc_column)

    for from_z in range(layers):
        @pl.when(z != from_z)
        def _(from_z=from_z):
            for s in range(sp_count):
                arrive(parts.at[from_z, s * tokens:(s + 1) * tokens], part_sem.at[from_z, s])
    raw = parts[0]
    for from_z in range(1, layers):
        raw = raw + parts[from_z]
    raw_keys = raw[:, :HEAD_DIM]
    key_heads = (
        raw_keys * cosines[...] + pltpu.roll(raw_keys, HEAD_DIM // 2, 1) * sines[...]
    ).astype(jnp.bfloat16)
    value_heads = raw[:, HEAD_DIM:].astype(jnp.bfloat16)
    factor = HEAD_DIM ** (-0.5)
    my_seq, my_head = z // per_half, y * per_half + z % per_half
    group_size = head_cols // HEAD_DIM
    outs = (out0, out1)
    for g in range(group_size):
        columns = slice(g * HEAD_DIM, (g + 1) * HEAD_DIM)
        scores = lax.dot_general(
            query_rows[:, columns], key_heads, (((1,), (1,)), ((), ())), preferred_element_type=jnp.float32
        ) * factor
        scores = jnp.where(allowed, scores, MASKED)
        highest = jnp.max(scores, axis=-1, keepdims=True)
        exponent = jnp.where(allowed, jnp.exp(scores - highest), 0.0)
        weights = (exponent / jnp.sum(exponent, axis=-1, keepdims=True)).astype(jnp.bfloat16)
        mixed[g] = jnp.dot(weights, value_heads, preferred_element_type=jnp.float32).astype(jnp.bfloat16)
        head = my_head * group_size + g
        out_columns = pl.ds(pl.multiple_of(head * HEAD_DIM, 128), HEAD_DIM)
        for s in range(sp_count):
            own = (sp == s) & (core == my_seq)
            for m in range(2):
                src = mixed.at[g, s * tokens:(s + 1) * tokens]
                dst, recv = outs[m].at[0, :, out_columns], out_sem.at[m, head]
                put(src, dst, recv, {"sp": s, "fsdp": my_seq}, (core == m) & jnp.logical_not(own))

                @pl.when((core == m) & own)
                def _(src=src, dst=dst, recv=recv):
                    pltpu.make_async_copy(src, dst, recv).start()
    for m in range(2):
        for head in range(2 * per_half * group_size):
            arrive(outs[m].at[0, :, head * HEAD_DIM:(head + 1) * HEAD_DIM], out_sem.at[m, head])
    for away, make in pending:
        if away is None:
            make().wait_send()
        else:
            @pl.when(away)
            def _(make=make):
                make().wait_send()


def fused(mesh, hiddens, queries, documents, gains, keys, values):
    sp = mesh.shape["sp"]
    tokens, features = hiddens[0].shape[1], keys[0].shape[0]
    kv_heads = keys[0].shape[1] // HEAD_DIM
    head_cols = queries[0].shape[2] // kv_heads
    layers, length, half = sp // 2, sp * tokens, keys[0].shape[1] // 2
    half_dim = HEAD_DIM // 2
    frequency = ROPE_BASE ** (-2.0 * np.arange(half_dim) / HEAD_DIM)
    angles = np.arange(length)[:, None] * frequency[None, :]
    cosines = np.concatenate([np.cos(angles), np.cos(angles)], axis=1).astype(np.float32)
    sines = np.concatenate([-np.sin(angles), np.sin(angles)], axis=1).astype(np.float32)
    dma = pltpu.SemaphoreType.DMA
    bf16, f32 = jnp.bfloat16, jnp.float32
    sends = 2 * layers + 12 + 4 * layers + 4 * kv_heads + layers + sp * layers
    group_size = head_cols // HEAD_DIM
    sends = sends + 2 + 2 * group_size * sp
    return pl.pallas_call(
        functools.partial(fused_kernel, sp),
        out_shape=(jax.ShapeDtypeStruct((1, tokens, queries[0].shape[2]), bf16),) * 2,
        in_specs=[pl.BlockSpec(memory_space=pltpu.VMEM)] * 14,
        out_specs=(pl.BlockSpec(memory_space=pltpu.VMEM),) * 2,
        scratch_shapes=[
            pltpu.VMEM((sp, 2 * tokens, 4 * features), bf16),
            pltpu.VMEM((4 * features, half), bf16),
            pltpu.VMEM((4 * features, half), bf16),
            pltpu.VMEM((2, 1, features), f32),
            pltpu.VMEM((2, 1, 128), f32),
            pltpu.VMEM((4, 1, features), f32),
            pltpu.VMEM((2, 1, 128), f32),
            pltpu.VMEM((2 * sp, 1, 128), f32),
            pltpu.VMEM((length, head_cols), bf16),
            pltpu.VMEM((sp, 1, 128), f32),
            pltpu.VMEM((sp * layers, tokens, 2 * HEAD_DIM), f32),
            pltpu.VMEM((layers, length, 2 * HEAD_DIM), f32),
            pltpu.VMEM((length, 128), f32),
            pltpu.VMEM((group_size, length, HEAD_DIM), bf16),
            dma((sends,)),
            dma((layers, 2)),
            dma((layers,)),
            dma((4, 2)),
            dma((4,)),
            dma((2 * sp,)),
            dma((sp,)),
            dma((sp,)),
            dma((layers, sp)),
            dma((2, kv_heads * group_size)),
        ],
        compiler_params=pltpu.CompilerParams(collective_id=0, has_side_effects=True),
        name="fused",
    )(
        *hiddens, *queries, *keys, *values,
        *gains, *documents, cosines, sines,
    )


def per_device(
    mesh,
    policy_hidden,
    policy_queries,
    policy_documents,
    policy_gain,
    policy_key_weight,
    policy_value_weight,
    frozen_hidden,
    frozen_queries,
    frozen_documents,
    frozen_gain,
    frozen_key_weight,
    frozen_value_weight,
):
    if fits(mesh, policy_hidden, policy_queries, policy_key_weight):
        return fused(
            mesh,
            (policy_hidden, frozen_hidden),
            (policy_queries, frozen_queries),
            (policy_documents, frozen_documents),
            (policy_gain, frozen_gain),
            (policy_key_weight, frozen_key_weight),
            (policy_value_weight, frozen_value_weight),
        )
    policy_mixed = run_model(
        policy_hidden,
        policy_queries,
        policy_documents,
        policy_gain,
        policy_key_weight,
        policy_value_weight,
    )
    frozen_mixed = run_model(
        frozen_hidden,
        frozen_queries,
        frozen_documents,
        frozen_gain,
        frozen_key_weight,
        frozen_value_weight,
    )
    return (policy_mixed, frozen_mixed)


def solution(mesh):
    return jax.shard_map(
        functools.partial(per_device, mesh),
        mesh=mesh,
        in_specs=(
            P(("groups", "fsdp"), "sp", None),
            P(("groups", "fsdp"), "sp", None),
            P(("groups", "fsdp"), "sp"),
            P(("sp", "fsdp")),
            P(("sp", "fsdp"), None),
            P(("sp", "fsdp"), None),
            P(("groups", "fsdp"), "sp", None),
            P(("groups", "fsdp"), "sp", None),
            P(("groups", "fsdp"), "sp"),
            P(("sp", "fsdp")),
            P(("sp", "fsdp"), None),
            P(("sp", "fsdp"), None),
        ),
        out_specs=(P(("groups", "fsdp"), "sp", None), P(("groups", "fsdp"), "sp", None)),
        check_vma=False,
    )
```

```python
import functools

import jax
import jax.numpy as jnp
import numpy as np
from jax import lax
from jax.experimental import pallas as pl
from jax.experimental.pallas import tpu as pltpu
from jax.sharding import PartitionSpec as P

HEAD_DIM = 128
LAG = 2


EPS = 1e-05
ROPE_BASE = 500000.0
MASKED = -1e30


def rotate(raw_keys, positions):
    half_dim = HEAD_DIM // 2
    frequency = jnp.exp(
        -jnp.log(ROPE_BASE) * jnp.arange(half_dim, dtype=jnp.float32) * 2.0 / HEAD_DIM
    )
    angles = positions.astype(jnp.float32)[:, None] * frequency[None, :]
    cosines = jnp.cos(angles)[:, None, :]
    sines = jnp.sin(angles)[:, None, :]
    front_half = raw_keys[..., :half_dim]
    back_half = raw_keys[..., half_dim:]
    return jnp.concatenate(
        [front_half * cosines - back_half * sines, back_half * cosines + front_half * sines],
        axis=-1,
    )


def project(hidden, gain, key_weight, value_weight):
    tokens = hidden.shape[1]
    widened = hidden[0].astype(jnp.float32)
    inverse = lax.rsqrt(jnp.mean(widened * widened, axis=-1, keepdims=True) + EPS)
    scaled = widened * inverse
    gain_rows = lax.all_gather(gain, ("sp", "fsdp"), axis=0, tiled=True)
    key_rows = lax.all_gather(key_weight, ("sp", "fsdp"), axis=0, tiled=True)
    value_rows = lax.all_gather(value_weight, ("sp", "fsdp"), axis=0, tiled=True)
    normed = (scaled * gain_rows.astype(jnp.float32)[None, :]).astype(jnp.bfloat16)
    raw_keys = jnp.dot(normed, key_rows, preferred_element_type=jnp.float32)
    raw_values = jnp.dot(normed, value_rows, preferred_element_type=jnp.float32)
    positions = lax.axis_index("sp") * tokens + jnp.arange(tokens, dtype=jnp.int32)
    key_heads = rotate(raw_keys.reshape(tokens, -1, HEAD_DIM), positions).astype(jnp.bfloat16)
    value_heads = raw_values.astype(jnp.bfloat16).reshape(tokens, -1, HEAD_DIM)
    return (key_heads, value_heads)


def attend(queries, key_heads, value_heads, documents):
    length = queries.shape[0]
    head_count = queries.shape[1]
    block_rows = min(512, length)
    margin = min(512, length // 2)
    window = block_rows + margin
    factor = HEAD_DIM ** (-0.5)
    offsets = jnp.arange(block_rows, dtype=jnp.int32)
    window_offsets = jnp.arange(window, dtype=jnp.int32)
    padding = jnp.zeros((margin, head_count, HEAD_DIM), jnp.bfloat16)
    padded_keys = jnp.concatenate([padding, key_heads], axis=0)
    padded_values = jnp.concatenate([padding, value_heads], axis=0)
    padded_docs = jnp.concatenate([jnp.full((margin,), -1, jnp.int32), documents], axis=0)

    def one_block(block_index):
        first = block_index * block_rows
        query_block = lax.dynamic_slice_in_dim(queries, first, block_rows, 0)
        query_docs = lax.dynamic_slice_in_dim(documents, first, block_rows, 0)
        query_positions = first + offsets
        key_block = lax.dynamic_slice_in_dim(padded_keys, first, window, 0)
        value_block = lax.dynamic_slice_in_dim(padded_values, first, window, 0)
        key_docs = lax.dynamic_slice_in_dim(padded_docs, first, window, 0)
        key_positions = first - margin + window_offsets
        allowed = (key_positions[None, :] <= query_positions[:, None]) & (
            key_docs[None, :] == query_docs[:, None]
        )
        scores = (
            jnp.einsum("qnd,knd->nqk", query_block, key_block, preferred_element_type=jnp.float32)
            * factor
        )
        scores = jnp.where(allowed[None], scores, MASKED)
        highest = jnp.max(scores, axis=-1, keepdims=True)
        exponent = jnp.where(allowed[None], jnp.exp(scores - highest), 0.0)
        weights = (exponent / jnp.sum(exponent, axis=-1, keepdims=True)).astype(jnp.bfloat16)
        blended = jnp.einsum(
            "nqk,knd->qnd", weights, value_block, preferred_element_type=jnp.float32
        )
        return blended.astype(jnp.bfloat16)

    blocks = lax.map(one_block, jnp.arange(length // block_rows, dtype=jnp.int32))
    return blocks.reshape(length, head_count, HEAD_DIM)


def run_model(hidden, queries, documents, gain, key_weight, value_weight):
    tokens = hidden.shape[1]
    head_count = queries.shape[2] // HEAD_DIM
    query_local = queries[0].reshape(tokens, head_count, HEAD_DIM)
    every_doc = lax.all_gather(documents[0], "sp", axis=0, tiled=True)
    key_heads, value_heads = project(hidden, gain, key_weight, value_weight)
    group_size = head_count // key_heads.shape[1]
    wide_keys = jnp.repeat(key_heads, group_size, axis=1)
    wide_values = jnp.repeat(value_heads, group_size, axis=1)
    query_spread, key_spread, value_spread = (
        lax.all_to_all(query_local, "sp", split_axis=1, concat_axis=0, tiled=True),
        lax.all_to_all(wide_keys, "sp", split_axis=1, concat_axis=0, tiled=True),
        lax.all_to_all(wide_values, "sp", split_axis=1, concat_axis=0, tiled=True),
    )
    mixed = attend(query_spread, key_spread, value_spread, every_doc)
    returned = lax.all_to_all(mixed, "sp", split_axis=0, concat_axis=1, tiled=True)
    return returned.reshape(1, tokens, head_count * HEAD_DIM)


MESH = pl.DeviceIdType.MESH


def fits(mesh, hidden, queries, key_weight):
    sp, cores = mesh.shape["sp"], mesh.shape["fsdp"]
    tokens = hidden.shape[1]
    kv_heads = key_weight.shape[1] // HEAD_DIM
    return (
        cores == 2
        and mesh.shape["groups"] == 2
        and sp % 2 == 0
        and kv_heads % 2 == 0
        and kv_heads == 4
        and sp // 2 == cores * (kv_heads // 2)
        and queries.shape[2] % (kv_heads * HEAD_DIM) == 0
        and key_weight.shape[0] % 128 == 0
        and hidden.shape[2] == key_weight.shape[0] * sp * cores
        and tokens % 16 == 0
        and tokens <= 128
    )


def fused_kernel(
    sp_count,
    hidden0, hidden1, queries0, queries1, key0, key1, value0, value1,
    gain0, gain1, documents0, documents1, cosines, sines,
    out0, out1,
    near, near_sem, rows, wide_k, wide_v, gains, documents, gain_rows, norm_send, norm_rows, query_rows, doc_rows,
    part_send, relayed, parts, doc_wide, mixed,
    send_sem, hid_sem, fwd_sem, w_sem, gain_sem, norm_sem, q_sem, doc_sem, part_sem, relay_sem, out_sem,
):
    hiddens, queries = (hidden0, hidden1), (queries0, queries1)
    keys, values = (key0, key1), (value0, value1)
    tokens, features = hidden0.shape[1], key0.shape[0]
    slab = 4 * features
    half = key0.shape[1] // 2
    per_half = half // HEAD_DIM
    head_cols = query_rows.shape[1]
    length = query_rows.shape[0]
    layers = sp_count // 2
    sp, core = lax.axis_index("sp"), lax.axis_index("fsdp")
    z, y = sp // 2, sp % 2
    group = lax.axis_index("groups")
    me = sp * 2 + core
    total = sp_count * 2

    for m in range(2):
        pltpu.make_async_copy(hiddens[m].at[0], near.at[m], near_sem.at[m]).start()
    barrier = pltpu.get_barrier_semaphore()
    for step in range(1, total):
        other = lax.rem(me + step, total)
        pl.semaphore_signal(
            barrier, inc=1, device_id={"sp": other // 2, "fsdp": other % 2}, device_id_type=MESH
        )

    pl.semaphore_signal(barrier, inc=1, device_id={"groups": 1 - group}, device_id_type=MESH)

    square = (
        lax.broadcasted_iota(jnp.int32, (tokens, 128), 0)
        == lax.broadcasted_iota(jnp.int32, (tokens, 128), 1)
    )
    for m in range(2):
        pltpu.make_async_copy(hiddens[m].at[0], near.at[m], near_sem.at[m]).wait()
        wide = near[m].astype(jnp.float32)
        inverse = lax.rsqrt(jnp.mean(wide * wide, axis=-1, keepdims=True) + EPS)
        gains[m] = (gain0, gain1)[m][...].astype(jnp.float32).reshape(1, -1)
        documents[m] = jnp.zeros((1, 128), jnp.float32)
        documents[m, :, :tokens] = (documents0, documents1)[m][...].astype(jnp.float32)
        norm_send[m] = jnp.sum(jnp.where(square, inverse, 0.0), axis=0, keepdims=True)

    pl.semaphore_wait(barrier, total)

    pending = []

    def remote(src, dst, recv, target):
        slot = len(pending)

        def make():
            return pltpu.make_async_remote_copy(
                src_ref=src, dst_ref=dst, send_sem=send_sem.at[slot], recv_sem=recv,
                device_id=target, device_id_type=MESH,
            )

        return make

    def put(src, dst, recv, target, away):
        make = remote(src, dst, recv, target)
        pending.append((away, make))
        if away is None:
            make().start()
        else:
            @pl.when(away)
            def _():
                make().start()

    def send(src, dst, recv, to_sp, to_core, own):
        put(src, dst, recv, {"sp": to_sp, "fsdp": to_core}, None if own is None else jnp.logical_not(own))
        if own is not None:
            @pl.when(own)
            def _():
                pltpu.make_async_copy(src, dst, recv).start()

    def arrive(dst, recv):
        pltpu.make_async_copy(dst, dst, recv).wait()

    for dz in range(layers):
        to_z = lax.rem(z + dz, layers)
        for m in range(2):
            send(
                hiddens[m].at[0, :, pl.ds(pl.multiple_of(to_z * slab, 128), slab)],
                rows.at[sp, pl.ds(pl.multiple_of(core * tokens, 16), tokens)],
                hid_sem.at[z, core],
                to_z * 2 + y, m,
                (core == m) if dz == 0 else None,
            )
    place = pl.ds(pl.multiple_of((y * 2 + core) * features, 128), features)
    for dy in (1, 0):
        to_y = (y + dy) % 2
        columns = pl.ds(pl.multiple_of(to_y * half, 128), half)
        for m in range(2):
            own = (core == m) if dy == 0 else None
            if dy:
                target = {"sp": z * 2 + to_y, "fsdp": m}
                put(keys[m].at[:, columns], wide_k.at[place], w_sem.at[y * 2 + core, 0], target, core == group)
                put(values[m].at[:, columns], wide_v.at[place], w_sem.at[y * 2 + core, 1], target, core == group)
            else:
                send(keys[m].at[:, columns], wide_k.at[place], w_sem.at[y * 2 + core, 0], z * 2 + to_y, m, own)
                send(values[m].at[:, columns], wide_v.at[place], w_sem.at[y * 2 + core, 1], z * 2 + to_y, m, own)
            send(gains.at[m], gain_rows.at[y * 2 + core], gain_sem.at[y * 2 + core], z * 2 + to_y, m, own)
    for dz in range(layers):
        for dy in range(2):
            to_sp = lax.rem(z + dz, layers) * 2 + (y + dy) % 2
            for m in range(2):
                send(
                    norm_send.at[m], norm_rows.at[me], norm_sem.at[me], to_sp, m,
                    (core == m) if dz == 0 and dy == 0 else None,
                )
    token_rows = pl.ds(pl.multiple_of(sp * tokens, 16), tokens)
    for b in range(per_half):
        for to_y in range(2):
            head = to_y * per_half + b
            to_sp = (core * per_half + b) * 2 + to_y
            for m in range(2):
                own = (to_sp == sp) & (core == m)
                send(
                    queries[m].at[0, :, head * head_cols:(head + 1) * head_cols],
                    query_rows.at[token_rows], q_sem.at[sp], to_sp, m, own,
                )
                send(documents.at[m], doc_rows.at[sp], doc_sem.at[sp], to_sp, m, own)

    for dz in range(layers):
        from_z = lax.rem(z - dz + layers, layers)
        block = from_z * 2 + y
        for c in range(2):
            arrive(rows.at[block, c * tokens:(c + 1) * tokens], hid_sem.at[from_z, c])
        send(rows.at[block], rows.at[block], fwd_sem.at[from_z], z * 2 + (1 - y), core, None)
        if dz < 2:
            source = (1 - y) * 2 + group
            wide = (wide_k, wide_v)[dz].at[pl.ds(pl.multiple_of(source * features, 128), features)]
            arrive(wide, w_sem.at[source, dz])
            put(wide, wide, w_sem.at[source, dz], {"groups": 1 - group}, None)

    for s in range(total):
        arrive(norm_rows.at[s], norm_sem.at[s])
    for s in range(4):
        arrive(gain_rows.at[s], gain_sem.at[s])
    for source in (y * 2, y * 2 + 1, (1 - y) * 2 + 1 - group):
        place = pl.ds(pl.multiple_of(source * features, 128), features)
        arrive(wide_k.at[place], w_sem.at[source, 0])
        arrive(wide_v.at[place], w_sem.at[source, 1])
    gain_row = jnp.concatenate([gain_rows[s] for s in range(4)], axis=1)

    inner = (z == per_half - 1) | (z == per_half)
    outer = jnp.logical_not(inner)
    neighbour = per_half - 1 + z // per_half

    def onward(index):
        block = (index % layers) * 2 + (y + index // layers) % 2
        block_rows = pl.ds(pl.multiple_of(block * tokens, 16), tokens)
        for to_z in range(layers):
            slot = index * layers + to_z
            away = inner & (z // per_half != to_z // per_half)

            @pl.when(away)
            def _(slot=slot):
                arrive(relayed.at[slot], relay_sem.at[slot])
                part_send[slot] = part_send[slot] + relayed[slot]

            put(
                part_send.at[slot], parts.at[z, block_rows], part_sem.at[z, block],
                {"sp": to_z * 2 + y, "fsdp": core}, away,
            )

    for index in range(2 * layers):
        from_z, side = index % layers, index // layers
        block = from_z * 2 + (y + side) % 2
        if side:
            arrive(rows.at[block], fwd_sem.at[from_z])
        scale = jnp.concatenate(
            [
                jnp.sum(jnp.where(square, norm_rows[block * 2 + c], 0.0), axis=1, keepdims=True)
                for c in range(2)
            ],
            axis=0,
        )
        normed = (rows[block].astype(jnp.float32) * scale * gain_row).astype(jnp.bfloat16)
        part_k = jnp.dot(normed, wide_k[...], preferred_element_type=jnp.float32)
        part_v = jnp.dot(normed, wide_v[...], preferred_element_type=jnp.float32)
        block_rows = pl.ds(pl.multiple_of(block * tokens, 16), tokens)
        for s in range(2):
            for b in range(per_half):
                to_z = s * per_half + b
                same = z // per_half == s
                picked = (slice(s * tokens, (s + 1) * tokens), slice(b * HEAD_DIM, (b + 1) * HEAD_DIM))
                slot = index * layers + to_z
                part_send[slot, :, :HEAD_DIM] = part_k[picked]
                part_send[slot, :, HEAD_DIM:] = part_v[picked]
                put(
                    part_send.at[slot], parts.at[z, block_rows], part_sem.at[z, block],
                    {"sp": to_z * 2 + y, "fsdp": core}, same & (z != to_z),
                )
                put(
                    part_send.at[slot], relayed.at[slot], relay_sem.at[slot],
                    {"sp": neighbour * 2 + y, "fsdp": core}, outer & jnp.logical_not(same),
                )

                @pl.when(z == to_z)
                def _(slot=slot, block_rows=block_rows):
                    parts[z, block_rows, :] = part_send[slot]

        if index >= LAG:
            onward(index - LAG)
    for index in range(2 * layers - LAG, 2 * layers):
        onward(index)

    for s in range(sp_count):
        arrive(query_rows.at[s * tokens:(s + 1) * tokens], q_sem.at[s])
        arrive(doc_rows.at[s], doc_sem.at[s])
        column = jnp.sum(jnp.where(square, doc_rows[s], 0.0), axis=1, keepdims=True)
        doc_wide[s * tokens:(s + 1) * tokens, :] = jnp.broadcast_to(column, (tokens, 128))
    query_index = lax.broadcasted_iota(jnp.int32, (length, length), 0)
    key_index = lax.broadcasted_iota(jnp.int32, (length, length), 1)
    doc_column = doc_wide[:, :1]
    doc_row = jnp.sum(jnp.where(query_index == key_index, doc_column, 0.0), axis=0, keepdims=True)
    allowed = (key_index <= query_index) & (doc_row == doc_column)

    def sent_by(from_z):
        if from_z in (per_half - 1, per_half):
            return z != from_z
        return (z != from_z) & (z // per_half == from_z // per_half)

    for from_z in range(layers):
        @pl.when(sent_by(from_z))
        def _(from_z=from_z):
            for s in range(sp_count):
                arrive(parts.at[from_z, s * tokens:(s + 1) * tokens], part_sem.at[from_z, s])
    raw = parts[z] + parts[z + 1 - 2 * (z % 2)] + parts[per_half - z // per_half]
    raw_keys = raw[:, :HEAD_DIM]
    key_heads = (
        raw_keys * cosines[...] + pltpu.roll(raw_keys, HEAD_DIM // 2, 1) * sines[...]
    ).astype(jnp.bfloat16)
    value_heads = raw[:, HEAD_DIM:].astype(jnp.bfloat16)
    factor = HEAD_DIM ** (-0.5)
    my_seq, my_head = z // per_half, y * per_half + z % per_half
    group_size = head_cols // HEAD_DIM
    outs = (out0, out1)
    for g in range(group_size):
        columns = slice(g * HEAD_DIM, (g + 1) * HEAD_DIM)
        scores = lax.dot_general(
            query_rows[:, columns], key_heads, (((1,), (1,)), ((), ())), preferred_element_type=jnp.float32
        ) * factor
        scores = jnp.where(allowed, scores, MASKED)
        highest = jnp.max(scores, axis=-1, keepdims=True)
        exponent = jnp.where(allowed, jnp.exp(scores - highest), 0.0)
        weights = (exponent / jnp.sum(exponent, axis=-1, keepdims=True)).astype(jnp.bfloat16)
        mixed[g] = jnp.dot(weights, value_heads, preferred_element_type=jnp.float32).astype(jnp.bfloat16)
        head = my_head * group_size + g
        out_columns = pl.ds(pl.multiple_of(head * HEAD_DIM, 128), HEAD_DIM)
        for s in range(sp_count):
            own = (sp == s) & (core == my_seq)
            for m in range(2):
                src = mixed.at[g, s * tokens:(s + 1) * tokens]
                dst, recv = outs[m].at[0, :, out_columns], out_sem.at[m, head]
                put(src, dst, recv, {"sp": s, "fsdp": my_seq}, (core == m) & jnp.logical_not(own))

                @pl.when((core == m) & own)
                def _(src=src, dst=dst, recv=recv):
                    pltpu.make_async_copy(src, dst, recv).start()
    for m in range(2):
        for head in range(2 * per_half * group_size):
            arrive(outs[m].at[0, :, head * HEAD_DIM:(head + 1) * HEAD_DIM], out_sem.at[m, head])
    for away, make in pending:
        if away is None:
            make().wait_send()
        else:
            @pl.when(away)
            def _(make=make):
                make().wait_send()


def fused(mesh, hiddens, queries, documents, gains, keys, values):
    sp = mesh.shape["sp"]
    tokens, features = hiddens[0].shape[1], keys[0].shape[0]
    kv_heads = keys[0].shape[1] // HEAD_DIM
    head_cols = queries[0].shape[2] // kv_heads
    layers, length, half = sp // 2, sp * tokens, keys[0].shape[1] // 2
    half_dim = HEAD_DIM // 2
    frequency = ROPE_BASE ** (-2.0 * np.arange(half_dim) / HEAD_DIM)
    angles = np.arange(length)[:, None] * frequency[None, :]
    cosines = np.concatenate([np.cos(angles), np.cos(angles)], axis=1).astype(np.float32)
    sines = np.concatenate([-np.sin(angles), np.sin(angles)], axis=1).astype(np.float32)
    dma = pltpu.SemaphoreType.DMA
    bf16, f32 = jnp.bfloat16, jnp.float32
    sends = 2 * layers + 12 + 4 * layers + 4 * kv_heads + layers + sp * layers
    group_size = head_cols // HEAD_DIM
    sends = sends + 2 + 2 * group_size * sp + 2 * sp * layers
    return pl.pallas_call(
        functools.partial(fused_kernel, sp),
        out_shape=(jax.ShapeDtypeStruct((1, tokens, queries[0].shape[2]), bf16),) * 2,
        in_specs=[pl.BlockSpec(memory_space=pl.ANY)] * 8 + [pl.BlockSpec(memory_space=pltpu.VMEM)] * 6,
        out_specs=(pl.BlockSpec(memory_space=pltpu.VMEM),) * 2,
        scratch_shapes=[
            pltpu.VMEM((2,) + hiddens[0].shape[1:], bf16),
            dma((2,)),
            pltpu.VMEM((sp, 2 * tokens, 4 * features), bf16),
            pltpu.VMEM((4 * features, half), bf16),
            pltpu.VMEM((4 * features, half), bf16),
            pltpu.VMEM((2, 1, features), f32),
            pltpu.VMEM((2, 1, 128), f32),
            pltpu.VMEM((4, 1, features), f32),
            pltpu.VMEM((2, 1, 128), f32),
            pltpu.VMEM((2 * sp, 1, 128), f32),
            pltpu.VMEM((length, head_cols), bf16),
            pltpu.VMEM((sp, 1, 128), f32),
            pltpu.VMEM((sp * layers, tokens, 2 * HEAD_DIM), f32),
            pltpu.VMEM((sp * layers, tokens, 2 * HEAD_DIM), f32),
            pltpu.VMEM((layers, length, 2 * HEAD_DIM), f32),
            pltpu.VMEM((length, 128), f32),
            pltpu.VMEM((group_size, length, HEAD_DIM), bf16),
            dma((sends,)),
            dma((layers, 2)),
            dma((layers,)),
            dma((4, 2)),
            dma((4,)),
            dma((2 * sp,)),
            dma((sp,)),
            dma((sp,)),
            dma((layers, sp)),
            dma((sp * layers,)),
            dma((2, kv_heads * group_size)),
        ],
        compiler_params=pltpu.CompilerParams(collective_id=0, has_side_effects=True),
        name="fused",
    )(
        *hiddens, *queries, *keys, *values,
        *gains, *documents, cosines, sines,
    )


def per_device(
    mesh,
    policy_hidden,
    policy_queries,
    policy_documents,
    policy_gain,
    policy_key_weight,
    policy_value_weight,
    frozen_hidden,
    frozen_queries,
    frozen_documents,
    frozen_gain,
    frozen_key_weight,
    frozen_value_weight,
):
    if fits(mesh, policy_hidden, policy_queries, policy_key_weight):
        return fused(
            mesh,
            (policy_hidden, frozen_hidden),
            (policy_queries, frozen_queries),
            (policy_documents, frozen_documents),
            (policy_gain, frozen_gain),
            (policy_key_weight, frozen_key_weight),
            (policy_value_weight, frozen_value_weight),
        )
    policy_mixed = run_model(
        policy_hidden,
        policy_queries,
        policy_documents,
        policy_gain,
        policy_key_weight,
        policy_value_weight,
    )
    frozen_mixed = run_model(
        frozen_hidden,
        frozen_queries,
        frozen_documents,
        frozen_gain,
        frozen_key_weight,
        frozen_value_weight,
    )
    return (policy_mixed, frozen_mixed)


def solution(mesh):
    return jax.shard_map(
        functools.partial(per_device, mesh),
        mesh=mesh,
        in_specs=(
            P(("groups", "fsdp"), "sp", None),
            P(("groups", "fsdp"), "sp", None),
            P(("groups", "fsdp"), "sp"),
            P(("sp", "fsdp")),
            P(("sp", "fsdp"), None),
            P(("sp", "fsdp"), None),
            P(("groups", "fsdp"), "sp", None),
            P(("groups", "fsdp"), "sp", None),
            P(("groups", "fsdp"), "sp"),
            P(("sp", "fsdp")),
            P(("sp", "fsdp"), None),
            P(("sp", "fsdp"), None),
        ),
        out_specs=(P(("groups", "fsdp"), "sp", None), P(("groups", "fsdp"), "sp", None)),
        check_vma=False,
    )
```
